32 devices in a mesh: seq: 32 (over z, y, x, core), tp: 1.
Axes of the slice: x: 2, y: 2, z: 4, core: 2. Of those that a mesh axis runs over, the one named last changes fastest.
Arguments:
- attn_out: bfloat16 [10240, 8192], P('seq', 'tp'), may hold values from -6 to 6
- out_weight: bfloat16 [8192, 8192], P('tp', 'seq'), may hold values from -0.0625 to 0.0625
- residual: bfloat16 [10240, 8192], P(('seq', 'tp')), may hold values from -114.6116 to 114.6116
- norm_gain: float32 [8192], replicated, may hold values from 0.5 to 1.5
- kv_weight: bfloat16 [8192, 2, 1024], P(None, None, 'tp'), may hold values from -0.0625 to 0.0625
Outputs:
- residual_out: bfloat16 [10240, 8192], P(('seq', 'tp'))
- quantized: bfloat16 [10240, 8192], P(('seq', 'tp'))
- peak: float32 [], replicated
- key_value: bfloat16 [10240, 2, 1024], P('seq', None, 'tp')
The draws below stay inside these ranges and needn't reach their ends.
All inputs are finite; a program needn't handle non-finite values. Where the reference program divides by a largest or mean magnitude, that divisor is 1e-20 or more.
Results may differ from the reference program's by a relative error of at most 0.014.
Values may be sent and summed in bfloat16 or wider, within the bound.
A program may use at most 256 MiB of HBM per device.

```python
import jax
import jax.numpy as jnp
from jax import lax

D = 8192
KVD = 1024
TOKENS = 10240
N_TP = 1


def draw_residual(key, part):
    first_key = jax.random.fold_in(key, 11)
    second_key = jax.random.fold_in(key, 12)
    third_key = jax.random.fold_in(key, 13)
    base = jnp.clip(jax.random.normal(first_key, (TOKENS, D), jnp.float32), -6.0, 6.0)
    low_end = 0.2
    high_end = 1.2
    column = jax.random.randint(second_key, (TOKENS,), 0, D)
    signs = (jax.random.randint(third_key, (TOKENS,), 0, 2) * 2 - 1).astype(jnp.float32)
    ramp = jnp.arange(TOKENS, dtype=jnp.float32) / max(TOKENS - 1, 1)
    magnitude = low_end * (high_end / low_end) ** ramp * D ** 0.5
    places = (jnp.arange(D)[None, :] == column[:, None]).astype(jnp.float32)
    return (base + places * (signs * magnitude)[:, None]).astype(jnp.bfloat16)


def shard_levels(own_key, shape, split, smallest, largest):
    factor_of, own = 1.0, jax.random.fold_in(own_key, 6)
    for axis_at, blocks in split:
        draws = jnp.exp(jax.random.uniform(jax.random.fold_in(own, axis_at), (blocks,), jnp.float32, smallest / len(split), largest / len(split)))
        factor_of = factor_of * jnp.repeat(draws, shape[axis_at] // blocks).reshape([-1 if axis == axis_at else 1 for axis in range(len(shape))])
    return factor_of


def normal_values(stream_key, extent, deviation, bound, cuts=(), held_as=jnp.bfloat16):
    entries = jax.random.normal(stream_key, extent, jnp.float32) * deviation
    if len(cuts) > 0:
        entries = shard_levels(stream_key, extent, cuts, -0.22, 0.18) * entries
    return jnp.clip(entries, min=-bound, max=bound).astype(held_as)


def setup_inputs(seed: int = 0) -> dict:
    keys = jax.random.split(jax.random.key(seed), 6)
    return {
        "attn_out": normal_values(keys[0], (TOKENS, D), 1.0, 6.0, ((0, 32),)),
        "out_weight": normal_values(keys[1], (D, D), D ** -0.5, 0.0625, ((1, 32),)),
        "residual": draw_residual(jax.random.fold_in(keys[5], 71), 0),
        "norm_gain": jnp.clip(1.0 + 0.1 * jax.random.normal(keys[3], (D,), jnp.float32), 0.5, 1.5),
        "kv_weight": normal_values(keys[4], (D, 2, KVD), D ** -0.5, 0.0625),
    }


def reference(attn_out, out_weight, residual, norm_gain, kv_weight):
    group_width = D // N_TP
    summed = jnp.zeros((TOKENS, D), jnp.float32)
    for group_index in range(N_TP):
        lower = group_index * group_width
        partial_value = jnp.dot(attn_out[:, lower:lower + group_width], out_weight[lower:lower + group_width, :], preferred_element_type=jnp.float32)
        summed = summed + lax.optimization_barrier(partial_value.astype(jnp.bfloat16)).astype(jnp.float32)
    hidden = residual.astype(jnp.float32) + summed
    mean_square = lax.optimization_barrier(jnp.mean(hidden * hidden, axis=1, keepdims=True))
    normed = (hidden * lax.rsqrt(mean_square + 1e-05) * norm_gain).astype(jnp.bfloat16)
    peak_value = jnp.max(jnp.abs(normed.astype(jnp.float32)))
    quantized = (normed.astype(jnp.float32) * (448.0 / peak_value)).astype(jnp.bfloat16)
    projected = jnp.dot(quantized, kv_weight.reshape(D, 2 * KVD), preferred_element_type=jnp.float32)
    key_value = (projected * (peak_value / 448.0)).astype(jnp.bfloat16).reshape(TOKENS, 2, KVD)
    return (hidden.astype(jnp.bfloat16), quantized, peak_value, key_value)
```

```python
import jax
import jax.numpy as jnp
from jax import lax
from jax.sharding import PartitionSpec as P

GROUP = 8


def normalize(hidden, norm_gain):
    mean_square = jnp.mean(hidden * hidden, axis=1, keepdims=True)
    return (hidden * lax.rsqrt(mean_square + 1e-05) * norm_gain).astype(jnp.bfloat16)


def group_rows(attn_out, kv_weight, n):
    def swap(value, bits):
        return lax.ppermute(value, "seq", [(s, s ^ bits) for s in range(n)])

    half = attn_out.shape[0] // 2
    core, x, y = 1, 2, 4
    over_x, over_y = swap(attn_out, x), swap(attn_out, y)
    over_x, kv_weight = lax.optimization_barrier((over_x, kv_weight))
    diagonal = jnp.concatenate([swap(over_x[:half], y), swap(over_y[half:], x)], axis=0)
    own = [attn_out, over_x, over_y, diagonal]
    other = [swap(block, core) for block in own]
    return [block for pair in zip(own, other) for block in pair], kv_weight


def line_blocks(block, line, n):
    at = lax.axis_index("seq") // GROUP
    arrived = {}
    up = down = block
    for step in range(1, line):
        up = lax.ppermute(
            up, "seq",
            [(s, s + GROUP) for s in range((step - 1) * GROUP, n - GROUP)],
        )
        down = lax.ppermute(
            down, "seq",
            [(s, s - GROUP) for s in range(GROUP, n - (step - 1) * GROUP)],
        )
        arrived[-step], arrived[step] = up, down
    order = [
        [d for step in range(1, line) for d in (-step, step) if 0 <= p + d < line]
        for p in range(line)
    ]
    slots = []
    for slot in range(line - 1):
        distances = [order[p][slot] for p in range(line)]
        chosen = arrived[distances[0]]
        for p in range(1, line):
            if any(distances[p] != distances[q] for q in range(p)):
                chosen = jnp.where(at == p, arrived[distances[p]], chosen)
            else:
                chosen = chosen
        source = at + jnp.array(distances, jnp.int32)[at]
        slots.append((chosen, source))
    return [(block, at)] + slots


def to_owners(product, n):
    low = lax.axis_index("seq") % GROUP
    shape = product.shape
    rows = product.reshape(2, 2, 2, shape[0] // GROUP, shape[1])
    for axis, bit in ((0, 4), (1, 2), (2, 1)):
        rows = jnp.where((low & bit) != 0, jnp.flip(rows, axis), rows)
    rows = rows.reshape(shape)
    groups = [[first + i for i in range(GROUP)] for first in range(0, n, GROUP)]
    return lax.all_to_all(rows, "seq", 0, 1, axis_index_groups=groups, tiled=True)


def project(attn_out, out_weight, kv_weight, n):
    line = n // GROUP
    blocks = line_blocks(out_weight, line, n)
    parts, kv_weight = group_rows(attn_out, kv_weight, n)
    rows = jnp.concatenate(parts, axis=0)
    cols = out_weight.shape[1]
    wide = GROUP * cols
    branch = jnp.zeros((attn_out.shape[0], line * wide), jnp.bfloat16)
    for weight, source in blocks[:-1]:
        product = jnp.dot(rows, weight, preferred_element_type=jnp.float32)
        piece = to_owners(product.astype(jnp.bfloat16), n)
        branch = lax.dynamic_update_slice(branch, piece, (0, source * wide))
    weight, source = blocks[-1]
    branch, weight = lax.optimization_barrier((branch, weight))
    product = jnp.dot(rows, weight, preferred_element_type=jnp.float32)
    piece = to_owners(product.astype(jnp.bfloat16), n)
    return lax.dynamic_update_slice(branch, piece, (0, source * wide)), kv_weight


def largest_of_all(value, n):
    def pair(bits):
        return [(s, s ^ bits) for s in range(n)]

    def shift(step):
        return [(s, (s + step) % n) for s in range(n)]

    value = lax.pmax(value, "tp")
    for perms in (
        [pair(bits) for bits in range(1, GROUP)],
        [shift(step) for step in range(GROUP, n, GROUP)],
    ):
        others = [lax.ppermute(value, "seq", perm) for perm in perms]
        for other in others:
            value = jnp.maximum(value, other)
    return value


def make_per_device(n):
    def per_device(attn_out, out_weight, residual, norm_gain, kv_weight):
        width = residual.shape[1]
        kv_cols = kv_weight.shape[2]
        kv_weight = kv_weight.reshape(width, 2 * kv_cols)
        branch, kv_weight = project(attn_out, out_weight, kv_weight, n)
        summed = lax.psum_scatter(
            branch, "tp", scatter_dimension=0, tiled=True
        ).astype(jnp.float32)
        hidden = residual.astype(jnp.float32) + summed
        normed = normalize(hidden, norm_gain)
        peak_value = largest_of_all(jnp.max(jnp.abs(normed.astype(jnp.float32))), n)
        quantized = (normed.astype(jnp.float32) * (448.0 / peak_value)).astype(jnp.bfloat16)
        normed_all = lax.all_gather(normed, "tp", axis=0, tiled=True)
        key_value = (
            jnp.dot(
                normed_all,
                kv_weight,
                preferred_element_type=jnp.float32,
            )
            .astype(jnp.bfloat16)
            .reshape(normed_all.shape[0], 2, kv_cols)
        )
        return (hidden.astype(jnp.bfloat16), quantized, peak_value, key_value)

    return per_device


def solution(mesh):
    return jax.shard_map(
        make_per_device(mesh.shape["seq"]),
        mesh=mesh,
        in_specs=(P("seq", "tp"), P("tp", "seq"), P(("seq", "tp"), None), P(), P(None, None, "tp")),
        out_specs=(P(("seq", "tp"), None), P(("seq", "tp"), None), P(), P("seq", None, "tp")),
        check_vma=False,
    )
```
